32 devices in a mesh: rep: 16 (over z, y, core), tp: 2 (over x).
Axes of the slice: x: 2, y: 2, z: 4, core: 2. Of those that a mesh axis runs over, the one named last changes fastest.
Arguments:
- positions: int32 [4096], P('rep'), may hold values from 0 to 8191
- activations: bfloat16 [4096, 4096], P('rep', 'tp'), may hold values from -6 to 6
- norm_gain: bfloat16 [4096], P('tp'), may hold values from 0.5 to 1.5
- qkv_weight: bfloat16 [4096, 6144], P('rep', 'tp'), may hold values from -0.09375 to 0.09375
- gate_up_weight: bfloat16 [4096, 14336], P('rep', 'tp'), may hold values from -0.09375 to 0.09375
Outputs:
- qkv_out: bfloat16 [4096, 6144], P('rep', 'tp')
- hidden: bfloat16 [4096, 7168], P('rep', 'tp')
The draws below stay inside these ranges and needn't reach their ends.
All inputs are finite; a program needn't handle non-finite values.
Results may differ from the reference program's by a relative error of at most 0.0058.
Values may be sent and summed in bfloat16 or wider, within the bound.
No kernel may reach another device: no remote copies, remote signals or barrier semaphores. Data moves between devices by JAX's collectives and lax.ppermute only.
A program may use at most 192 MiB of HBM per device.

```python
import jax
import jax.numpy as jnp
from jax import lax

D = 4096
QH = 32
KVH = 8
HD = 128
FF = 7168
QKV = 6144
TOTAL_SEQS = 4096
N_TP = 2


def with_ends(entries, rng, smallest, largest):
    shape = entries.shape
    index_at = [jax.random.randint(jax.random.fold_in(rng, axis), (), 0, shape[axis]) for axis in range(len(shape))]
    entries = entries.at[tuple(index_at)].set(smallest)
    longest = shape.index(max(shape))
    index_at[longest] = (index_at[longest] + 1) % shape[longest]
    return entries.at[tuple(index_at)].set(largest)


def steps_of(rng, extent, pieces, low, largest):
    def one(axis_at, shards_of):
        heights = jax.random.uniform(jax.random.fold_in(jax.random.fold_in(rng, 6), axis_at), (shards_of,), jnp.float32, low / len(pieces), largest / len(pieces))
        return jnp.repeat(jnp.exp(heights), extent[axis_at] // shards_of).reshape((-1,) + (1,) * (len(extent) - axis_at - 1))

    loudness = one(*pieces[0])
    for cut in pieces[1:]:
        loudness = loudness * one(*cut)
    return loudness


def gaussian(key, shape, scale, most, pieces=(), kind=jnp.bfloat16):
    entries = scale * jax.random.normal(key, shape, jnp.float32)
    if pieces:
        entries = entries * steps_of(key, shape, pieces, -0.22, 0.18)
    return jnp.clip(entries, -most, most).astype(kind)


def setup_inputs(seed: int = 0) -> dict:
    seeds = jax.random.split(jax.random.key(seed), 6)
    return {
        "positions": with_ends(jax.random.randint(seeds[0], (TOTAL_SEQS,), 0, 8192), jax.random.fold_in(seeds[0], 1), 0, 8191).astype(jnp.int32),
        "activations": gaussian(seeds[1], (TOTAL_SEQS, D), 1.0, 6.0, ((0, 16), (1, 2))),
        "norm_gain": jnp.clip(1.0 + 0.1 * jax.random.normal(seeds[2], (D,), jnp.float32), 0.5, 1.5).astype(jnp.bfloat16),
        "qkv_weight": gaussian(seeds[3], (D, QKV), D ** -0.5, 0.09375, ((0, 16), (1, 2))),
        "gate_up_weight": gaussian(seeds[4], (D, 2 * FF), D ** -0.5, 0.09375, ((0, 16), (1, 2))),
    }


theta_base = 500000.0
norm_eps = 1e-05

def normalize(gathered, gain_row):
    values = gathered.astype(jnp.float32)
    mean_square = lax.optimization_barrier(jnp.mean(values * values, axis=1, keepdims=True))
    return (values * lax.rsqrt(mean_square + norm_eps) * gain_row.astype(jnp.float32)).astype(jnp.bfloat16)

def rotary(joined_qkv, positions):
    row_count = joined_qkv.shape[0]
    per_group = QH // KVH + 2
    half_size = HD // 2
    head_view = joined_qkv.reshape(row_count, -1, per_group, HD)
    frequency = theta_base ** (-2.0 * jnp.arange(half_size, dtype=jnp.float32) / HD)
    angles = positions.astype(jnp.float32)[:, None] * frequency[None, :]
    cosine = jnp.cos(angles)[:, None, None, :]
    sine_part = jnp.sin(angles)[:, None, None, :]
    leading = head_view[..., :half_size]
    trailing = head_view[..., half_size:]
    turned = jnp.concatenate([leading * cosine - trailing * sine_part, trailing * cosine + leading * sine_part], axis=-1)
    rotated_mask = (jnp.arange(per_group) < per_group - 1)[None, None, :, None]
    return jnp.where(rotated_mask, turned, head_view).reshape(row_count, -1)

def reference(positions, activations, norm_gain, qkv_weight, gate_up_weight):
    normed = normalize(activations, norm_gain)
    joined_qkv = jnp.dot(normed, qkv_weight, preferred_element_type=jnp.float32)
    qkv_out = rotary(joined_qkv, positions).astype(jnp.bfloat16)
    gate_up = jnp.dot(normed, gate_up_weight, preferred_element_type=jnp.float32)
    row_count = gate_up.shape[0]
    paired = gate_up.reshape(row_count, N_TP, 2, FF // N_TP)
    hidden = (jax.nn.silu(paired[:, :, 0]) * paired[:, :, 1]).reshape(row_count, FF).astype(jnp.bfloat16)
    return (qkv_out, hidden)
```

```python
import jax
import jax.numpy as jnp
from jax import lax
from jax.sharding import PartitionSpec as P

QH = 32
KVH = 8
HD = 128
CORES = 2
LANES = 128

theta_base = 500000.0
norm_eps = 1e-05


def exchange(value, axis, size, mask):
    return lax.ppermute(value, axis, [(i, i ^ mask) for i in range(size)])


def block_count(rep_size, head_count, unit_count):
    for blocks in (4, 2):
        if (rep_size // CORES) % blocks == 0 and head_count % blocks == 0 and unit_count % blocks == 0:
            return blocks
    return 1


def unit_chunks(units):
    first = min(units, -(-units // (2 * LANES)) * LANES)
    return [n for n in (first, units - first) if n]


def rotary(joined, cosine, sine, head_base):
    rows = joined.shape[0]
    per_group = QH // KVH + 2
    half = HD // 2
    view = joined.reshape(rows, -1, HD)
    a, b = view[..., :half], view[..., half:]
    cos, sin = cosine[:, None, :], sine[:, None, :]
    turned = jnp.concatenate([a * cos - b * sin, b * cos + a * sin], axis=-1)
    head = (head_base + jnp.arange(view.shape[1])) % per_group
    return jnp.where((head < per_group - 1)[None, :, None], turned, view).reshape(rows, -1)


def make(mesh):
    rep_size, tp_size = mesh.shape["rep"], mesh.shape["tp"]
    pairs = rep_size // CORES

    def per_device(positions, activations, norm_gain, qkv_weight, gate_up_weight):
        rep, tp = lax.axis_index("rep"), lax.axis_index("tp")
        seqs, feats = activations.shape
        rows = qkv_weight.shape[0]
        units = gate_up_weight.shape[1] // 2
        heads = qkv_weight.shape[1] // HD
        blocks = block_count(rep_size, heads, units)
        chip, core = rep // CORES, rep % CORES
        mine = chip % blocks

        acts, gains, where_at = activations, norm_gain, positions
        bit = blocks // 2
        parts, spots = [acts], [where_at]
        bit = 1
        while bit < blocks:
            got = exchange(jnp.concatenate(parts, 0), "rep", rep_size, bit * CORES)
            spot = exchange(jnp.concatenate(spots, 0), "rep", rep_size, bit * CORES)
            parts, spots = parts + [got], spots + [spot]
            bit *= 2
        acts = jnp.concatenate(parts, 0)
        where_at = jnp.concatenate(spots, 0)
        all_acts = [acts] + [exchange(acts, "tp", tp_size, k) for k in range(1, tp_size)]
        all_gains = [gains] + [exchange(gains, "tp", tp_size, k) for k in range(1, tp_size)]

        square = 0.0
        for part in all_acts:
            part = part.astype(jnp.float32)
            square = square + jnp.sum(part * part, axis=1, keepdims=True)
        scale = lax.rsqrt(square / (feats * tp_size) + norm_eps)
        normed = jnp.stack(
            [
                (v.astype(jnp.float32) * scale * g.astype(jnp.float32)).astype(jnp.bfloat16)
                for v, g in zip(all_acts, all_gains)
            ]
        )
        per_tp = rep_size // tp_size
        slabs = []
        for other in range(CORES):
            for k in range(pairs):
                source = (chip ^ k) * CORES + (core ^ other)
                slabs.append(
                    lax.dynamic_slice(
                        normed,
                        (tp ^ (source // per_tp), 0, (source % per_tp) * rows),
                        (1, normed.shape[1], rows),
                    )[0]
                )
        chosen = jnp.concatenate(slabs, axis=1)

        half = HD // 2
        frequency = theta_base ** (-2.0 * jnp.arange(half, dtype=jnp.float32) / HD)
        angles = where_at.astype(jnp.float32)[:, None] * frequency[None, :]
        cosine, sine = jnp.cos(angles), jnp.sin(angles)

        head_block, unit_block = heads // blocks, units // blocks

        def pieces_of(cut):
            sends = [cut(mine ^ k) for k in range(blocks)]
            pieces = [None] * pairs
            for k in list(range(blocks, pairs)) + list(range(1, blocks)):
                pieces[k] = exchange(sends[k % blocks], "rep", rep_size, k * CORES)
            pieces[0] = sends[0]
            others = [exchange(v, "rep", rep_size, 1) for v in pieces]
            return jnp.concatenate(pieces + others, axis=0)

        def deliver(out):
            got = [out[:seqs]]
            for k in range(1, blocks):
                got.append(exchange(out[k * seqs : (k + 1) * seqs], "rep", rep_size, k * CORES))
            stacked = jnp.stack(got)
            return [
                lax.dynamic_index_in_dim(stacked, mine ^ b, 0, keepdims=False)
                for b in range(blocks)
            ]

        width = head_block * HD
        weight = pieces_of(
            lambda b: lax.dynamic_slice(qkv_weight, (0, b * width), (rows, width))
        )
        joined = jnp.dot(chosen, weight, preferred_element_type=jnp.float32)
        turned = rotary(joined, cosine, sine, mine * head_block).astype(jnp.bfloat16)
        qkv_out = jnp.concatenate(deliver(turned), axis=1)

        done = []
        start = 0
        for count in unit_chunks(unit_block):

            def cut(b, start=start, count=count):
                at = b * unit_block + start
                return jnp.concatenate(
                    [
                        lax.dynamic_slice(gate_up_weight, (0, at), (rows, count)),
                        lax.dynamic_slice(gate_up_weight, (0, units + at), (rows, count)),
                    ],
                    axis=1,
                )

            both = jnp.dot(chosen, pieces_of(cut), preferred_element_type=jnp.float32)
            unit = (jax.nn.silu(both[:, :count]) * both[:, count:]).astype(jnp.bfloat16)
            done.append(deliver(unit))
            start += count
        hidden = jnp.concatenate(
            [part[b] for b in range(blocks) for part in done], axis=1
        )
        return (qkv_out, hidden)

    return per_device


def solution(mesh):
    placed = (P("rep"), P("rep", "tp"), P("tp"), P("rep", "tp"), P("rep", "tp"))
    return jax.shard_map(
        make(mesh),
        mesh=mesh,
        in_specs=placed,
        out_specs=(P("rep", "tp"), P("rep", "tp")),
        check_vma=False,
    )
```

```python
import jax
import jax.numpy as jnp
from jax import lax
from jax.sharding import PartitionSpec as P

QH = 32
KVH = 8
HD = 128
CORES = 2
LANES = 128

theta_base = 500000.0
norm_eps = 1e-05


def exchange(value, axis, size, mask):
    return lax.ppermute(value, axis, [(i, i ^ mask) for i in range(size)])


def block_count(rep_size, head_count, unit_count):
    for blocks in (4, 2):
        if (rep_size // CORES) % blocks == 0 and head_count % blocks == 0 and unit_count % blocks == 0:
            return blocks
    return 1


def unit_chunks(units):
    first = min(units, -(-7 * units // (10 * LANES)) * LANES)
    return [n for n in (first, units - first) if n]


def rotary(joined, cosine, sine, head_base):
    rows = joined.shape[0]
    per_group = QH // KVH + 2
    half = HD // 2
    view = joined.reshape(rows, -1, HD)
    a, b = view[..., :half], view[..., half:]
    cos, sin = cosine[:, None, :], sine[:, None, :]
    turned = jnp.concatenate([a * cos - b * sin, b * cos + a * sin], axis=-1)
    head = (head_base + jnp.arange(view.shape[1])) % per_group
    return jnp.where((head < per_group - 1)[None, :, None], turned, view).reshape(rows, -1)


def make(mesh):
    rep_size, tp_size = mesh.shape["rep"], mesh.shape["tp"]
    pairs = rep_size // CORES

    def per_device(positions, activations, norm_gain, qkv_weight, gate_up_weight):
        rep, tp = lax.axis_index("rep"), lax.axis_index("tp")
        seqs, feats = activations.shape
        rows = qkv_weight.shape[0]
        units = gate_up_weight.shape[1] // 2
        heads = qkv_weight.shape[1] // HD
        blocks = block_count(rep_size, heads, units)
        chip, core = rep // CORES, rep % CORES
        mine = chip % blocks

        def after(values, gate):
            return values if gate is None else lax.optimization_barrier((values, gate))[0]

        head_block, unit_block = heads // blocks, units // blocks
        width = head_block * HD

        def qkv_cut(b):
            return lax.dynamic_slice(qkv_weight, (0, b * width), (rows, width))

        def unit_cut(start, count):
            def cut(b):
                at = b * unit_block + start
                return jnp.concatenate(
                    [
                        lax.dynamic_slice(gate_up_weight, (0, at), (rows, count)),
                        lax.dynamic_slice(gate_up_weight, (0, units + at), (rows, count)),
                    ],
                    axis=1,
                )

            return cut

        def send_far(cut, gate):
            sends = after([cut(mine ^ k) for k in range(blocks)], gate)
            pieces = [sends[0]] + [None] * (pairs - 1)
            for k in range(blocks, pairs):
                pieces[k] = exchange(sends[k % blocks], "rep", rep_size, k * CORES)
            return sends, pieces

        def send_near(sends, pieces, gate):
            sends = after(sends, gate)
            for k in range(1, blocks):
                pieces[k] = exchange(sends[k], "rep", rep_size, k * CORES)

        qkv_sends, qkv_pieces = send_far(qkv_cut, None)
        begun = qkv_pieces[blocks] if pairs > blocks else None

        parts, spots = {0: after(activations, qkv_sends)}, {0: positions}
        hops = []
        bit = blocks // 2
        while bit:
            held = {j: after(v, begun) if hops else v for j, v in parts.items()}
            for j in list(parts):
                parts[j ^ bit] = exchange(held[j], "rep", rep_size, bit * CORES)
                spots[j ^ bit] = exchange(spots[j], "rep", rep_size, bit * CORES)
            hops.append([v for j, v in parts.items() if j & bit])
            bit //= 2
        where_at = jnp.concatenate([spots[j] for j in range(blocks)], 0)
        all_acts = [jnp.concatenate([parts[j] for j in range(blocks)], 0)]
        all_gains = [norm_gain]
        for k in range(1, tp_size):
            swapped = [exchange(parts[j], "tp", tp_size, k) for j in range(blocks)]
            all_acts.append(jnp.concatenate(swapped, 0))
            all_gains.append(exchange(norm_gain, "tp", tp_size, k))

        first = hops[0] if hops else None
        last = hops[-1] if hops else None
        send_near(qkv_sends, qkv_pieces, first)
        counts = unit_chunks(unit_block)
        unit_pieces = []
        start = 0
        for count in counts:
            sends, pieces = send_far(unit_cut(start, count), last if start else first)
            send_near(sends, pieces, last if start else first)
            unit_pieces.append(pieces)
            start += count

        half = HD // 2
        frequency = theta_base ** (-2.0 * jnp.arange(half, dtype=jnp.float32) / HD)
        angles = where_at.astype(jnp.float32)[:, None] * frequency[None, :]
        cosine, sine = jnp.cos(angles), jnp.sin(angles)
        all_acts, cosine, sine = lax.optimization_barrier((all_acts, cosine, sine))

        square = 0.0
        for part in all_acts:
            part = part.astype(jnp.float32)
            square = square + jnp.sum(part * part, axis=1, keepdims=True)
        scale = lax.rsqrt(square / (feats * tp_size) + norm_eps)
        normed = jnp.stack(
            [
                (v.astype(jnp.float32) * scale * g.astype(jnp.float32)).astype(jnp.bfloat16)
                for v, g in zip(all_acts, all_gains)
            ]
        )
        per_tp = rep_size // tp_size
        slabs = []
        for other in range(CORES):
            for k in range(pairs):
                source = (chip ^ k) * CORES + (core ^ other)
                slabs.append(
                    lax.dynamic_slice(
                        normed,
                        (tp ^ (source // per_tp), 0, (source % per_tp) * rows),
                        (1, normed.shape[1], rows),
                    )[0]
                )
        chosen = [
            jnp.concatenate(slabs[half * pairs : (half + 1) * pairs], axis=1)
            for half in range(CORES)
        ]

        def project(pieces, gate):
            own = jnp.concatenate(after(pieces, gate), axis=0)
            other = exchange(own, "rep", rep_size, 1)
            total = jnp.dot(chosen[0], own, preferred_element_type=jnp.float32)
            return total + jnp.dot(chosen[1], other, preferred_element_type=jnp.float32)

        def deliver(out):
            got = [out[:seqs]]
            for k in range(1, blocks):
                got.append(exchange(out[k * seqs : (k + 1) * seqs], "rep", rep_size, k * CORES))
            return got

        def in_order(got, gate):
            stacked = jnp.stack(after(got, gate))
            return [
                lax.dynamic_index_in_dim(stacked, mine ^ b, 0, keepdims=False)
                for b in range(blocks)
            ]

        joined = project(qkv_pieces, last)
        turned = rotary(joined, cosine, sine, mine * head_block).astype(jnp.bfloat16)
        qkv_parts = deliver(turned)

        done, gate = [], (turned, unit_pieces[-1][-pairs // 2])
        for count, pieces in zip(counts, unit_pieces):
            both = project(pieces, gate)
            unit = (jax.nn.silu(both[:, :count]) * both[:, count:]).astype(jnp.bfloat16)
            done.append(deliver(unit))
            gate = (unit, turned)
        qkv_out = jnp.concatenate(in_order(qkv_parts, gate[0]), axis=1)
        done = [in_order(got, gate[0]) for got in done]
        hidden = jnp.concatenate(
            [part[b] for b in range(blocks) for part in done], axis=1
        )
        return (qkv_out, hidden)

    return per_device


def solution(mesh):
    placed = (P("rep"), P("rep", "tp"), P("tp"), P("rep", "tp"), P("rep", "tp"))
    return jax.shard_map(
        make(mesh),
        mesh=mesh,
        in_specs=placed,
        out_specs=(P("rep", "tp"), P("rep", "tp")),
        check_vma=False,
    )
```
